1024 devices in a mesh: dp: 16 (over y, x_hi), expert: 64 (over z, x_lo, core).
Axes of the slice: x: 4 (x_hi: 2, x_lo: 2; x = x_hi * 2 + x_lo), y: 8, z: 16, core: 2. Of those that a mesh axis runs over, the one named last changes fastest.
Arguments:
- tokens: bfloat16 [2048, 4096], P('expert', 'dp'), may hold values from -6 to 6
- cotangent: bfloat16 [2048, 4096], P('expert', 'dp'), may hold values from -6 to 6
- expert_ids: int32 [2048, 8], P('expert'), may hold values from 0 to 47, all different within a row; in each aligned block of 32 rows (0 to 31, 32 to 63, ...) at most 6 rows name the same one
- gate_weights: float32 [2048, 8], P('expert'), may hold values from 0.2 to 1
- slot_table: int32 [64], replicated, may hold values from 0 to 47, as said below
- split_count: int32 [48], replicated, may hold values from 0 to 64
- w_gate: bfloat16 [64, 4096, 768], P('expert', 'dp'), may hold values from -0.09375 to 0.09375
- w_up: bfloat16 [64, 4096, 768], P('expert', 'dp'), may hold values from -0.09375 to 0.09375
- w_down: bfloat16 [64, 768, 4096], P('expert', None, 'dp'), may hold values from -0.21875 to 0.21875
Outputs:
- mixed: bfloat16 [2048, 4096], P('expert', 'dp')
- token_grad: bfloat16 [2048, 4096], P('expert', 'dp')
- gate_grad: bfloat16 [64, 4096, 768], P('expert', 'dp')
- up_grad: bfloat16 [64, 4096, 768], P('expert', 'dp')
- down_grad: bfloat16 [64, 768, 4096], P('expert', None, 'dp')
The draws below stay inside these ranges and needn't reach their ends.
Inputs may be any that keep to these rules, and one draw needn't show every extreme that they name: `expert_ids`: in the rows of one device (aligned blocks of 32 rows), no expert is named more than 6 times. `slot_table`: every expert is held by one or two slots; exactly 16 experts are held by two, and those sit on slots s and s + 32 with s below 32.
All inputs are finite; a program needn't handle non-finite values.
Results may differ from the reference program's by a relative error of at most 0.028.
Values may be sent and summed in bfloat16 or wider, within the bound.
A program may use at most 32 MiB of HBM per device.

```python
import math
import jax
import jax.numpy as jnp
import numpy as np
from jax import lax

D = 4096
FF = 768
TOK_DEV = 32
TOKENS = 2048
SLOTS = 64
HOT = 16
EXPERTS = 48
TOP = 8
CAP = 6
N_DP = 16
N_EXPERT = 64


def draw_slot_table(key, part):
    order = jax.random.permutation(jax.random.fold_in(key, 11), EXPERTS).astype(jnp.int32)
    half_count = SLOTS // 2
    ranking = jax.random.permutation(jax.random.fold_in(key, 12), half_count)
    doubled = ranking < HOT
    cold_rank = jnp.cumsum(jnp.logical_not(doubled).astype(jnp.int32)) - 1
    second_index = jnp.where(doubled, jnp.arange(half_count, dtype=jnp.int32), half_count + cold_rank)
    second_half = order[second_index]
    return jnp.concatenate([order[:half_count], second_half]).astype(jnp.int32)


def touch_ends(drawn, stream_key, least, high):
    place = [jax.random.randint(jax.random.fold_in(stream_key, axis), (), 0, length) for axis, length in enumerate(drawn.shape)]
    widest = drawn.shape.index(max(drawn.shape))
    next_to = place[:widest] + [(place[widest] + 1) % drawn.shape[widest]] + place[widest + 1:]
    return drawn.at[tuple(place)].set(least).at[tuple(next_to)].set(high)


def level_of(own_key, extent, split, low, largest):
    gain = 1.0
    for dim, blocks in split:
        steps = jax.random.uniform(jax.random.fold_in(jax.random.fold_in(own_key, 6), dim), (blocks,), jnp.float32, low / len(split), largest / len(split))
        gain = gain * jnp.repeat(jnp.exp(steps), extent[dim] // blocks).reshape((-1,) + (1,) * (len(extent) - 1 - dim))
    return gain


def deal_out(stream_key, own, number, rows, amount, top, bound, lean):
    order = jax.random.permutation(stream_key, amount)
    heavy_load, usual = load_shares(amount, rows * top, bound, lean, True), load_shares(amount, rows * top, bound, lean, False)
    places = jnp.arange(amount)

    def named(tallies, turn):
        used = int((tallies > 0).sum())
        fixed = max(1, used // 4)
        shifted = fixed + (places - fixed + turn * (used - fixed)) % max(1, amount - fixed)
        return jnp.zeros((amount,), jnp.int32).at[order[jnp.where(places < fixed, places, shifted)]].set(jnp.asarray(tallies, jnp.int32))

    tallies = jnp.where(number % 4 == 0, named(heavy_load, number // 4), named(usual, number - number // 4 - 1))
    mixed = jax.random.permutation(jax.random.fold_in(own, 3), amount)
    giver, receiver = mixed[0:amount // 2 * 2:2], mixed[1:amount // 2 * 2:2]
    margin = jnp.minimum(tallies[giver] - 1, bound - tallies[receiver]) // 2
    margin = jnp.where((giver == order[0]) | (receiver == order[0]) | (tallies[receiver] == 0), 0, jnp.maximum(margin, 0))
    shifted = jax.random.randint(jax.random.fold_in(own, 4), (amount // 2,), 0, 1 << 20) % (margin + 1)
    tallies = tallies.at[giver].add(-shifted).at[receiver].add(shifted)
    items = jnp.searchsorted(jnp.cumsum(tallies), jnp.arange(rows * top), side="right").astype(jnp.int32)
    grid = items.reshape(top, rows).T
    grid = grid[jax.random.permutation(jax.random.fold_in(own, 1), rows)]
    turn = jax.random.randint(jax.random.fold_in(own, 2), (rows, 1), 0, top)
    return jnp.take_along_axis(grid, (jnp.arange(top)[None, :] + turn) % top, axis=1)


def load_shares(number_of, total, most, lean, full):
    weights = [(1 << 20) // math.isqrt(grade ** lean) + 1 for grade in range(1, number_of + 1)]
    largest = most if full else min(most, max(-(-total // number_of), total * weights[0] // sum(weights)))
    least = 1 if total - largest >= number_of - 1 else 0
    holding, surplus = [largest] + [least] * (number_of - 1), total - largest - least * (number_of - 1)
    while surplus > 0:
        movable = [i for i in range(1, number_of) if holding[i] < largest] or [i for i in range(1, number_of) if holding[i] < most]
        pool, remaining = sum([weights[i] for i in movable]), surplus
        for i in movable:
            addition = min(most - holding[i], max(1, remaining * weights[i] // pool), surplus)
            holding[i] = holding[i] + addition
            surplus = surplus - addition
    return np.array(holding)


def bell_draw(key, extent, width, bound, cuts=(), kind=jnp.bfloat16):
    entries = width * jax.random.normal(key, extent, jnp.float32)
    if cuts:
        entries = entries * level_of(key, extent, cuts, -0.22, 0.18)
    return jnp.clip(entries, -bound, bound).astype(kind)


def setup_inputs(seed: int = 0) -> dict:
    streams_of = jax.random.split(jax.random.key(seed), 10)
    tokens = bell_draw(streams_of[0], (TOKENS, D), 1.0, 6.0, ((0, 64), (1, 16)))
    cotangent = bell_draw(streams_of[1], (TOKENS, D), 0.5, 6.0, ((0, 64), (1, 16)))
    expert_ids_keys = jax.random.split(jax.random.fold_in(streams_of[2], 1), TOKENS // TOK_DEV)
    expert_ids_turns = jax.random.permutation(jax.random.fold_in(streams_of[2], 3), TOKENS // TOK_DEV)
    expert_ids = jax.vmap(lambda own, number: deal_out(jax.random.fold_in(streams_of[2], 2), own, number, TOK_DEV, EXPERTS, TOP, CAP, 2))(expert_ids_keys, expert_ids_turns).reshape((TOKENS, TOP))
    gate_weights = jnp.clip(0.2 + 0.8 * jax.random.uniform(streams_of[3], (TOKENS, TOP), jnp.float32) ** level_of(streams_of[3], (TOKENS, TOP), ((0, 64),), -0.2, 0.2), 0.2, 1.0)
    slot_table = draw_slot_table(jax.random.fold_in(streams_of[9], 71), 0)
    split_count = touch_ends(jax.random.randint(streams_of[5], (EXPERTS,), 0, N_EXPERT + 1), jax.random.fold_in(streams_of[5], 1), 0, N_EXPERT).astype(jnp.int32)
    w_gate = bell_draw(streams_of[6], (SLOTS, D, FF), D ** -0.5, 0.09375, ((0, 64), (1, 16)))
    w_up = bell_draw(streams_of[7], (SLOTS, D, FF), D ** -0.5, 0.09375, ((0, 64), (1, 16)))
    w_down = bell_draw(streams_of[8], (SLOTS, FF, D), FF ** -0.5, 0.21875, ((0, 64), (2, 16)))
    return {"tokens": tokens, "cotangent": cotangent, "expert_ids": expert_ids, "gate_weights": gate_weights, "slot_table": slot_table, "split_count": split_count, "w_gate": w_gate, "w_up": w_up, "w_down": w_down}


def slot_choice(expert_ids, slot_table, split_count, source):
    slot_count = slot_table.shape[0]
    expert_count = split_count.shape[0]
    slot_iota = jnp.arange(slot_count, dtype=jnp.int32)
    expert_iota = jnp.arange(expert_count, dtype=jnp.int32)
    holds = slot_table[None, :] == expert_iota[:, None]
    lower = jnp.min(jnp.where(holds, slot_iota[None, :], slot_count), axis=1)
    upper = jnp.max(jnp.where(holds, slot_iota[None, :], -1), axis=1)
    chosen = jnp.where(source < split_count, lower, upper).astype(jnp.int32)
    flat_ids = expert_ids.reshape(-1)
    matches = flat_ids[:, None] == expert_iota[None, :]
    target = jnp.sum(jnp.where(matches, chosen[None, :], 0), axis=1).astype(jnp.int32)
    onehot = (target[:, None] == slot_iota[None, :]).astype(jnp.int32)
    before = jnp.cumsum(onehot, axis=0) - onehot
    position = jnp.sum(before * onehot, axis=1).astype(jnp.int32)
    return target, position


def swiglu(gate_pre, up_pre):
    return (jax.nn.silu(gate_pre) * up_pre).astype(jnp.bfloat16)


def swiglu_back(gate_pre, up_pre, upstream):
    sigma = jax.nn.sigmoid(gate_pre)
    gate_back = upstream * up_pre * sigma * (1.0 + gate_pre * (1.0 - sigma))
    up_back = upstream * gate_pre * sigma
    return gate_back.astype(jnp.bfloat16), up_back.astype(jnp.bfloat16)


def shard_sum(left, right_mat, form):
    parts = jnp.einsum(form, left.astype(jnp.float32), right_mat.astype(jnp.float32))
    rounded = lax.optimization_barrier(parts.astype(jnp.bfloat16))
    return jnp.sum(rounded.astype(jnp.float32), axis=0)


def pair_total(grads, paired):
    partner_grads = jnp.roll(grads, SLOTS // 2, axis=0).astype(jnp.float32)
    return (grads.astype(jnp.float32) + paired[:, None, None] * partner_grads).astype(jnp.bfloat16)


def reference(tokens, cotangent, expert_ids, gate_weights, slot_table, split_count, w_gate, w_up, w_down):
    slot_rows = N_EXPERT * CAP
    shard_width = D // N_DP
    sources = jnp.arange(N_EXPERT, dtype=jnp.int32)
    grouped_ids = expert_ids.reshape(N_EXPERT, TOK_DEV, TOP)

    def place_one(group_ids, source_id):
        return slot_choice(group_ids, slot_table, split_count, source_id)

    target, position = jax.vmap(place_one)(grouped_ids, sources)
    assigned = jnp.arange(TOKENS * TOP, dtype=jnp.int32).reshape(N_EXPERT, TOK_DEV * TOP)
    source_grid = jnp.broadcast_to(sources[:, None], assigned.shape)
    layout = jnp.full((SLOTS, N_EXPERT, CAP), -1, dtype=jnp.int32)
    layout = layout.at[target, source_grid, position].set(assigned).reshape(SLOTS, slot_rows)
    gate_flat = gate_weights.reshape(-1)

    def slot_pass(carry, item):
        mixed_sum, token_sum = carry
        index, gate_mat, up_mat, down_mat = item
        valid = index >= 0
        safe = jnp.where(valid, index, 0).astype(jnp.int32)
        token = (safe // TOP).astype(jnp.int32)
        weight = jnp.where(valid, gate_flat[safe], 0.0)
        slot_in = jnp.where(valid[:, None], tokens[token], jnp.zeros((), jnp.bfloat16))
        slot_back = (weight[:, None] * cotangent[token].astype(jnp.float32)).astype(jnp.bfloat16)
        split_in = slot_in.reshape(slot_rows, N_DP, shard_width)
        gate_pre = shard_sum(split_in, gate_mat.reshape(N_DP, shard_width, FF), "rnd,ndf->nrf")
        up_pre = shard_sum(split_in, up_mat.reshape(N_DP, shard_width, FF), "rnd,ndf->nrf")
        hidden_act = swiglu(gate_pre, up_pre)
        slot_out = jnp.dot(hidden_act, down_mat, preferred_element_type=jnp.float32).astype(jnp.bfloat16)
        upstream = shard_sum(slot_back.reshape(slot_rows, N_DP, shard_width), down_mat.reshape(FF, N_DP, shard_width), "rnd,fnd->nrf")
        gate_back, up_back = swiglu_back(gate_pre, up_pre, upstream)
        grad_gate = jnp.dot(slot_in.T, gate_back, preferred_element_type=jnp.float32).astype(jnp.bfloat16)
        grad_up = jnp.dot(slot_in.T, up_back, preferred_element_type=jnp.float32).astype(jnp.bfloat16)
        grad_down = jnp.dot(hidden_act.T, slot_back, preferred_element_type=jnp.float32).astype(jnp.bfloat16)
        slot_dx = jnp.dot(gate_back, gate_mat.T, preferred_element_type=jnp.float32)
        slot_dx = (slot_dx + jnp.dot(up_back, up_mat.T, preferred_element_type=jnp.float32)).astype(jnp.bfloat16)
        mixed_sum = mixed_sum.at[token].add(weight[:, None] * slot_out.astype(jnp.float32))
        token_sum = token_sum.at[token].add(jnp.where(valid[:, None], slot_dx.astype(jnp.float32), 0.0))
        return (mixed_sum, token_sum), (grad_gate, grad_up, grad_down)

    start = (jnp.zeros((TOKENS, D), jnp.float32), jnp.zeros((TOKENS, D), jnp.float32))
    (mixed_sum, token_sum), (grad_gate, grad_up, grad_down) = lax.scan(slot_pass, start, (layout, w_gate, w_up, w_down))
    paired = (slot_table == jnp.roll(slot_table, SLOTS // 2)).astype(jnp.float32)
    return (mixed_sum.astype(jnp.bfloat16), token_sum.astype(jnp.bfloat16), pair_total(grad_gate, paired), pair_total(grad_up, paired), pair_total(grad_down, paired))
```

```python
import functools

import jax
import jax.numpy as jnp
from jax import lax
from jax.experimental import pallas as pl
from jax.experimental.pallas import tpu as pltpu
from jax.sharding import PartitionSpec as P

MESH = pl.DeviceIdType.MESH
BF16 = jnp.bfloat16
F32 = jnp.float32
PAD = 8


def contract(a, b, da, db):
    return lax.dot_general(a, b, (((da,), (db,)), ((), ())), preferred_element_type=F32)


def near_order(count):
    return sorted(range(1, count), key=lambda k: (-min(k, count - k), k))


def layer_kernel(
    dims,
    bounds, ids, gates, lane_expert, lane_chosen, tok, cot, wg, wu, wd,
    mixed, tgrad, ggrad, ugrad, dgrad,
    send_tok, send_cot, send_out, send_dx, got_tok, got_cot, got_out, got_dx,
    slot_in, slot_back, w_high, w_low, own_sel,
    part_gu, part_u, xr_gu, xr_u, ys_gu, ys_u, yr_gu, yr_u, share, far, full,
    flat_send, flat_recv, x_send, x_recv, y_send, y_recv, z_send, z_recv,
    gy_send, gy_recv, gx_send, gx_recv,
):
    n_dp, n_exp, cap, top = dims
    n_y = n_dp // 2
    tokens, width = tok.shape
    rows = n_exp * cap
    lanes = n_exp * PAD
    block, cols = share.shape[1:]
    me = lax.axis_index("expert")
    place = lax.axis_index("dp")
    yy = lax.div(place, 2)
    xx = lax.rem(place, 2)
    other_x = 1 - xx
    x_peer = yy * 2 + other_x
    z_peer = lax.rem(me + n_exp // 2, n_exp)

    def y_at(k):
        return lax.rem(yy + k, n_y)

    barrier = pltpu.get_barrier_semaphore()

    def greet(k, carry):
        pl.semaphore_signal(
            barrier, inc=1, device_id={"expert": lax.rem(me + k, n_exp)}, device_id_type=MESH
        )
        return carry

    lax.fori_loop(1, n_exp, greet, 0)
    pl.semaphore_signal(barrier, inc=1, device_id={"dp": x_peer}, device_id_type=MESH)
    for k in range(1, n_y):
        pl.semaphore_signal(barrier, inc=1, device_id={"dp": y_at(k) * 2 + xx}, device_id_type=MESH)

    shape = (tokens, lanes)
    held = jnp.zeros(shape, jnp.int32)
    weight = jnp.zeros(shape, F32)
    slot_expert = jnp.broadcast_to(lane_expert[...], shape)
    for k in range(top):
        hit = jnp.broadcast_to(ids[:, k : k + 1], shape) == slot_expert
        held = jnp.where(hit, 1, held)
        weight = jnp.where(hit, jnp.broadcast_to(gates[:, k : k + 1], shape), weight)
    t_row = lax.broadcasted_iota(jnp.int32, (tokens, tokens), 0)
    t_col = lax.broadcasted_iota(jnp.int32, (tokens, tokens), 1)
    earlier = jnp.where(t_col < t_row, 1.0, 0.0).astype(BF16)
    position = contract(earlier, held.astype(F32).astype(BF16), 1, 0)
    rank = jnp.bitwise_and(lax.broadcasted_iota(jnp.int32, shape, 1), PAD - 1).astype(F32)
    at_rank = jnp.where(position == rank, held, 0).astype(F32)
    chosen = at_rank * jnp.broadcast_to(lane_chosen[...], shape).astype(F32)
    own_weight = chosen * weight
    high = own_weight.astype(BF16)
    w_high[...] = high
    w_low[...] = (own_weight - high.astype(F32)).astype(BF16)
    own_sel[...] = chosen.astype(BF16)
    select = at_rank.astype(BF16)
    send_tok[...] = contract(select, tok[...], 0, 0).reshape(n_exp, PAD, width).astype(BF16)
    row_weight = jnp.sum(at_rank * weight, axis=0, keepdims=True)
    row_weight = jnp.transpose(jnp.broadcast_to(row_weight, (128, lanes)))[:, :1]
    back = contract(select, cot[...], 0, 0) * row_weight
    send_cot[...] = back.reshape(n_exp, PAD, width).astype(BF16)

    pl.semaphore_wait(barrier, n_exp - 1 + 1 + n_y - 1)

    def scatter(src, dst, at):
        def one(i, carry):
            turn = n_exp - i
            half = lax.div(turn + 1, 2)
            odd = lax.rem(turn, 2)
            peer = lax.rem(me + odd * half + (1 - odd) * (n_exp - half), n_exp)
            pltpu.make_async_remote_copy(
                src_ref=src.at[peer],
                dst_ref=dst.at[me],
                send_sem=flat_send.at[at],
                recv_sem=flat_recv.at[at],
                device_id={"expert": peer},
                device_id_type=MESH,
            ).start()
            return carry

        lax.fori_loop(1, n_exp, one, 0)
        dst[me] = src[me]

    def wait_bytes(ref, sem):
        pltpu.make_async_copy(ref, ref, sem).wait()

    def wait_scatter(dst, at):
        wait_bytes(dst.at[pl.ds(0, n_exp - 1)], flat_recv.at[at])

    scatter(send_tok, got_tok, 0)
    scatter(send_cot, got_cot, 1)

    def matching(shape, row_dim):
        row = lax.broadcasted_iota(jnp.int32, shape, row_dim)
        col = lax.broadcasted_iota(jnp.int32, shape, 1 - row_dim)
        rank = jnp.bitwise_and(col, PAD - 1)
        at = jnp.right_shift(col, 3) * cap + rank
        return jnp.where(at == row, jnp.where(rank < cap, 1.0, 0.0), 0.0).astype(BF16)

    def flat(ref):
        return ref[...].astype(F32).reshape(lanes, width).astype(BF16)

    pack = matching((rows, lanes), 0)
    wait_scatter(got_tok, 0)
    slot_in[...] = contract(pack, flat(got_tok), 1, 0).astype(BF16)

    def put(dst, which, value):
        value = value.astype(BF16)
        for h in range(2):
            dst[h, :, which] = value[:, h * cols : (h + 1) * cols].reshape(n_y, block, cols)

    put(part_gu, 0, contract(slot_in[...], wg[...], 1, 0))
    put(part_gu, 1, contract(slot_in[...], wu[...], 1, 0))

    turns = near_order(n_y)

    def x_stage(part, landing, at):
        for k in turns + [0]:
            b = y_at(k)
            pltpu.make_async_remote_copy(
                src_ref=part.at[other_x, b],
                dst_ref=landing.at[b],
                send_sem=x_send.at[at],
                recv_sem=x_recv.at[at, b],
                device_id={"dp": x_peer},
                device_id_type=MESH,
            ).start()

    def x_sum(part, landing, at, b):
        wait_bytes(landing.at[b], x_recv.at[at, b])
        return part[xx, b].astype(F32) + landing[b].astype(F32)

    def y_stage(part, landing, out, there, at):
        for k in turns:
            b = y_at(k)
            out[b] = x_sum(part, landing, at, b).astype(BF16)
            pltpu.make_async_remote_copy(
                src_ref=out.at[b],
                dst_ref=there.at[yy],
                send_sem=y_send.at[at],
                recv_sem=y_recv.at[at],
                device_id={"dp": b * 2 + xx},
                device_id_type=MESH,
            ).start()
        there[yy] = x_sum(part, landing, at, yy).astype(BF16)

    def y_sum(there, at):
        wait_bytes(there.at[pl.ds(0, n_y - 1)], y_recv.at[at])
        total = there[0].astype(F32)
        for b in range(1, n_y):
            total = total + there[b].astype(F32)
        return total

    x_stage(part_gu, xr_gu, 0)
    y_stage(part_gu, xr_gu, ys_gu, yr_gu, 0)

    wait_scatter(got_cot, 1)
    slot_back[...] = contract(pack, flat(got_cot), 1, 0).astype(BF16)
    put(part_u, 0, contract(slot_back[...], wd[...], 1, 1))
    x_stage(part_u, xr_u, 1)
    y_stage(part_u, xr_u, ys_u, yr_u, 1)

    def z_copy(m):
        return pltpu.make_async_remote_copy(
            src_ref=share.at[m],
            dst_ref=far.at[m],
            send_sem=z_send.at[m],
            recv_sem=z_recv.at[m],
            device_id={"expert": z_peer},
            device_id_type=MESH,
        )

    both = y_sum(yr_gu, 0)
    gate_pre, up_pre = both[0], both[1]
    sigma = 1.0 / (1.0 + jnp.exp(-gate_pre))
    share[0] = (gate_pre * sigma * up_pre).astype(BF16)
    z_copy(0).start()
    upstream = y_sum(yr_u, 1)[0]
    share[1] = (upstream * up_pre * sigma * (1.0 + gate_pre * (1.0 - sigma))).astype(BF16)
    share[2] = (upstream * gate_pre * sigma).astype(BF16)
    z_copy(1).start()
    z_copy(2).start()

    row = lax.broadcasted_iota(jnp.int32, (block, cols), 0) + yy * block
    owned = jnp.where(row >= bounds[0], jnp.where(row < bounds[1], 1, 0), 0)

    def to_y(m):
        z_copy(m).wait_recv()
        mine = jnp.where(owned > 0, share[m].astype(F32), far[m].astype(F32))
        full[m, xx, yy] = mine.astype(BF16)
        for k in turns:
            b = y_at(k)
            pltpu.make_async_remote_copy(
                src_ref=full.at[m, xx, yy],
                dst_ref=full.at[m, xx, yy],
                send_sem=gy_send.at[m],
                recv_sem=gy_recv.at[m, yy],
                device_id={"dp": b * 2 + xx},
                device_id_type=MESH,
            ).start()
        to_x(m, yy)

    def to_x(m, b):
        pltpu.make_async_remote_copy(
            src_ref=full.at[m, xx, b],
            dst_ref=full.at[m, xx, b],
            send_sem=gx_send.at[m],
            recv_sem=gx_recv.at[m],
            device_id={"dp": x_peer},
            device_id_type=MESH,
        ).start()

    def pass_on(m):
        for k in reversed(turns):
            b = y_at(k)
            wait_bytes(full.at[m, xx, b], gy_recv.at[m, b])
            to_x(m, b)

    def whole(m, h):
        return full[m, h].reshape(rows, cols)

    def product(m, mat, dim):
        wait_bytes(full.at[m, other_x], gx_recv.at[m])
        total = None
        for h in range(2):
            cut = mat[h * cols : (h + 1) * cols, :] if dim == 0 else mat[:, h * cols : (h + 1) * cols]
            term = contract(whole(m, h), cut, 1, dim)
            total = term if total is None else total + term
        return total

    spread = matching((lanes, rows), 1)

    def give(value, src, dst, at):
        src[...] = contract(spread, value.astype(BF16), 1, 0).reshape(n_exp, PAD, width).astype(BF16)
        scatter(src, dst, at)

    to_y(0)
    to_y(1)
    to_y(2)
    pass_on(0)
    pass_on(1)
    give(product(0, wd, 0), send_out, got_out, 2)
    pass_on(2)
    dx = product(1, wg, 1)
    give(dx + product(2, wu, 1), send_dx, got_dx, 3)
    for h in range(2):
        cut = slice(h * cols, (h + 1) * cols)
        ggrad[:, cut] = contract(slot_in[...], whole(1, h), 0, 0).astype(BF16)
        ugrad[:, cut] = contract(slot_in[...], whole(2, h), 0, 0).astype(BF16)
        dgrad[cut, :] = contract(whole(0, h), slot_back[...], 0, 0).astype(BF16)

    wait_scatter(got_out, 2)
    out_rows = flat(got_out)
    mixed[...] = (contract(w_high[...], out_rows, 1, 0) + contract(w_low[...], out_rows, 1, 0)).astype(BF16)
    wait_scatter(got_dx, 3)
    tgrad[...] = contract(own_sel[...], flat(got_dx), 1, 0).astype(BF16)

    for at, src in enumerate((send_tok, send_cot, send_out, send_dx)):
        wait_bytes(src.at[pl.ds(0, n_exp - 1)], flat_send.at[at])
    for at, (part, out) in enumerate(((part_gu, ys_gu), (part_u, ys_u))):
        wait_bytes(part.at[0], x_send.at[at])
        wait_bytes(out.at[pl.ds(0, n_y - 1)], y_send.at[at])
    for m in range(3):
        z_copy(m).wait_send()
        wait_bytes(full.at[m, xx, pl.ds(0, n_y - 1)], gy_send.at[m])
        wait_bytes(full.at[m, xx], gx_send.at[m])


def on_device(
    tokens, cotangent, expert_ids, gate_weights, slot_table, split_count, w_gate, w_up, w_down
):
    slot_count = slot_table.shape[0]
    expert_count = split_count.shape[0]
    token_count, top_k = expert_ids.shape
    width = tokens.shape[1]
    hidden_width = w_gate.shape[2]
    cap = max(2, (token_count * top_k + expert_count - 1) // expert_count)
    n_dp = lax.axis_size("dp")
    n_exp = slot_count
    source = lax.axis_index("expert")
    half = slot_count // 2
    n_y = n_dp // 2
    rows = n_exp * cap
    block = rows // n_y
    cols = hidden_width // 2
    lanes = n_exp * PAD

    doubled = slot_table == jnp.roll(slot_table, half)
    experts = jnp.arange(expert_count, dtype=jnp.int32)
    split_at = jnp.sum(jnp.where(slot_table[:, None] == experts[None, :], split_count[None, :], 0), axis=1)
    lower = jnp.arange(slot_count, dtype=jnp.int32) < half
    start = jnp.where(doubled & jnp.logical_not(lower), split_at, 0)
    end = jnp.where(doubled & lower, split_at, n_exp)
    chosen = ((source >= start) & (source < end)).astype(jnp.int32)
    lane_expert = jnp.repeat(slot_table, PAD)[None, :]
    lane_chosen = jnp.repeat(chosen, PAD)[None, :]
    bounds = lax.dynamic_index_in_dim(jnp.stack([start, end], 1) * cap, source, 0, keepdims=False)

    vm = pl.BlockSpec(memory_space=pltpu.VMEM)
    message = pltpu.VMEM((n_exp, PAD, width), BF16)

    def halves(*lead):
        return pltpu.VMEM((*lead, block, cols), BF16)

    dma = pltpu.SemaphoreType.DMA
    mixed, tgrad, ggrad, ugrad, dgrad = pl.pallas_call(
        functools.partial(layer_kernel, (n_dp, n_exp, cap, top_k)),
        out_shape=(
            jax.ShapeDtypeStruct((token_count, width), BF16),
            jax.ShapeDtypeStruct((token_count, width), BF16),
            jax.ShapeDtypeStruct((width, hidden_width), BF16),
            jax.ShapeDtypeStruct((width, hidden_width), BF16),
            jax.ShapeDtypeStruct((hidden_width, width), BF16),
        ),
        in_specs=[pl.BlockSpec(memory_space=pltpu.SMEM)] + [vm] * 9,
        out_specs=(vm,) * 5,
        scratch_shapes=[
            *([message] * 8),
            pltpu.VMEM((rows, width), BF16),
            pltpu.VMEM((rows, width), BF16),
            *([pltpu.VMEM((token_count, lanes), BF16)] * 3),
            halves(2, n_y, 2),
            halves(2, n_y, 1),
            *([halves(n_y, 2), halves(n_y, 1)] * 3),
            halves(3),
            halves(3),
            halves(3, 2, n_y),
            dma((4,)),
            dma((4,)),
            dma((2,)),
            dma((2, n_y)),
            dma((2,)),
            dma((2,)),
            dma((3,)),
            dma((3,)),
            dma((3,)),
            dma((3, n_y)),
            dma((3,)),
            dma((3,)),
        ],
        compiler_params=pltpu.CompilerParams(collective_id=0, has_side_effects=True),
        name="expert_layer",
    )(
        bounds, expert_ids, gate_weights, lane_expert, lane_chosen, tokens, cotangent,
        w_gate[0], w_up[0], w_down[0],
    )
    return mixed, tgrad, ggrad[None], ugrad[None], dgrad[None]


def solution(mesh):
    return jax.shard_map(
        on_device,
        mesh=mesh,
        in_specs=(
            P("expert", "dp"),
            P("expert", "dp"),
            P("expert", None),
            P("expert", None),
            P(),
            P(),
            P("expert", "dp", None),
            P("expert", "dp", None),
            P("expert", None, "dp"),
        ),
        out_specs=(
            P("expert", "dp"),
            P("expert", "dp"),
            P("expert", "dp", None),
            P("expert", "dp", None),
            P("expert", None, "dp"),
        ),
        check_vma=False,
    )
```

```python
import functools

import jax
import jax.numpy as jnp
from jax import lax
from jax.experimental import pallas as pl
from jax.experimental.pallas import tpu as pltpu
from jax.sharding import PartitionSpec as P

MESH = pl.DeviceIdType.MESH
BF16 = jnp.bfloat16
F32 = jnp.float32
PAD = 4
SHIFT = 2


def contract(a, b, da, db):
    return lax.dot_general(a, b, (((da,), (db,)), ((), ())), preferred_element_type=F32)


def near_order(count):
    return sorted(range(1, count), key=lambda k: (-min(k, count - k), k))


def layer_kernel(
    dims,
    table, splits, ids, gates, tok, cot, wg, wu, wd,
    mixed, tgrad, ggrad, ugrad, dgrad,
    send_tok, send_cot, send_out, send_dx, got_tok, got_cot, got_out, got_dx,
    slot_in, slot_back, w_high, w_low, own_sel, turned, limits,
    *rest,
):
    products, landed, passed, terms = (rest[4 * i : 4 * i + 4] for i in range(4))
    share, far, full = (rest[16 + 2 * i : 18 + 2 * i] for i in range(3))
    (
        flat_send, flat_recv, x_send, x_recv, y_send, y_recv, z_send, z_recv,
        gy_send, gy_recv, gx_send, gx_recv,
    ) = rest[22:]
    n_dp, n_exp, cap, top = dims
    assert cap == PAD + 2
    n_y = n_dp // 2
    tokens, width = tok.shape
    rows = n_exp * cap
    lanes = n_exp * PAD
    block = share[0].shape[1]
    widths = [ref.shape[2] for ref in share]
    cols = sum(widths)
    begins = [0, widths[0]]
    me = lax.axis_index("expert")
    place = lax.axis_index("dp")
    yy = lax.div(place, 2)
    xx = lax.rem(place, 2)
    other_x = 1 - xx
    x_peer = yy * 2 + other_x
    z_peer = lax.rem(me + n_exp // 2, n_exp)

    def y_at(k):
        return lax.rem(yy + k, n_y)

    barrier = pltpu.get_barrier_semaphore()

    def greet(k, carry):
        pl.semaphore_signal(
            barrier, inc=1, device_id={"expert": lax.rem(me + k, n_exp)}, device_id_type=MESH
        )
        return carry

    lax.fori_loop(1, n_exp, greet, 0)
    pl.semaphore_signal(barrier, inc=1, device_id={"dp": x_peer}, device_id_type=MESH)
    for k in range(1, n_y):
        pl.semaphore_signal(barrier, inc=1, device_id={"dp": y_at(k) * 2 + xx}, device_id_type=MESH)

    def lane_of_slot(shift):
        slot = lax.broadcasted_iota(jnp.int32, (n_exp, lanes), 0) + shift
        slot = jnp.where(slot >= n_exp, slot - n_exp, slot)
        lane = jnp.right_shift(lax.broadcasted_iota(jnp.int32, (n_exp, lanes), 1), SHIFT)
        return jnp.where(slot == lane, 1.0, 0.0).astype(BF16)

    def small(ref):
        return jnp.broadcast_to(ref[...].astype(F32), (8, ref.shape[1])).astype(BF16)

    slot_expert = contract(small(table), lane_of_slot(0), 1, 0)
    other_expert = contract(small(table), lane_of_slot(n_exp // 2), 1, 0)
    experts = splits.shape[1]
    expert = lax.broadcasted_iota(jnp.int32, (experts, lanes), 0).astype(F32)
    named = jnp.where(expert == jnp.broadcast_to(slot_expert[:1], (experts, lanes)), 1.0, 0.0)
    split_at = contract(small(splits), named.astype(BF16), 1, 0)
    lane = lax.broadcasted_iota(jnp.int32, (8, lanes), 1)
    alone = slot_expert != other_expert
    start = jnp.where(alone, 0.0, jnp.where(lane < lanes // 2, 0.0, split_at))
    end = jnp.where(alone, float(n_exp), jnp.where(lane < lanes // 2, split_at, float(n_exp)))
    mine = me.astype(F32)
    lane_chosen = jnp.where(start <= mine, jnp.where(mine < end, 1.0, 0.0), 0.0)
    for i, limit in enumerate((start, end)):
        at_me = jnp.sum(jnp.where(lane == me * PAD, limit, 0.0), axis=1, keepdims=True)
        limits[i] = jnp.broadcast_to(at_me * cap, (8, cols))

    turned[...] = jnp.zeros(turned.shape, F32)
    turned[0:top, 0:tokens] = ids[...].astype(F32)
    turned[top : 2 * top, 0:tokens] = gates[...]
    columns = jnp.transpose(turned[...])[:tokens]
    shape = (tokens, lanes)
    held = jnp.zeros(shape, F32)
    weight = jnp.zeros(shape, F32)
    wanted = jnp.broadcast_to(slot_expert[:1], shape)
    for k in range(top):
        hit = jnp.broadcast_to(columns[:, k : k + 1], shape) == wanted
        held = jnp.where(hit, 1.0, held)
        weight = jnp.where(hit, jnp.broadcast_to(columns[:, top + k : top + k + 1], shape), weight)
    t_row = lax.broadcasted_iota(jnp.int32, (tokens, tokens), 0)
    t_col = lax.broadcasted_iota(jnp.int32, (tokens, tokens), 1)
    earlier = jnp.where(t_col < t_row, 1.0, 0.0).astype(BF16)
    position = contract(earlier, held.astype(BF16), 1, 0)
    turn = jnp.bitwise_and(lax.broadcasted_iota(jnp.int32, shape, 1), PAD - 1)
    ranks = (turn, jnp.bitwise_and(turn, 1) + PAD)
    at_rank = [jnp.where(position == rank.astype(F32), held, 0.0) for rank in ranks]
    left = jnp.where(turn < 2, 1.0, 0.0)
    at_rank = [at_rank[0], at_rank[1] * left, at_rank[1] * (1.0 - left)]
    chosen = jnp.broadcast_to(lane_chosen[:1], shape)
    for i, at in enumerate(at_rank):
        own_weight = at * chosen * weight
        high = own_weight.astype(BF16)
        w_high[i] = high
        w_low[i] = (own_weight - high.astype(F32)).astype(BF16)
        own_sel[i] = (at * chosen).astype(BF16)
    piece = width // 2

    def folded(picks, value, da):
        whole_rows = contract(picks[0], value, da, 0)
        halves = contract(picks[1], value[:, :piece], da, 0) + contract(picks[2], value[:, piece:], da, 0)
        return whole_rows, halves

    def message(whole_rows, halves):
        both = jnp.concatenate([whole_rows, halves], axis=1)
        return both.reshape(n_exp, PAD, width + piece).astype(BF16)

    picks = [at.astype(BF16) for at in at_rank]
    send_tok[...] = message(*folded(picks, tok[...], 0))

    def row_weight(at):
        row = jnp.sum(at * weight, axis=0, keepdims=True)
        return jnp.transpose(jnp.broadcast_to(row, (128, lanes)))[:, :1]

    whole_rows, halves = folded(picks, cot[...], 0)
    send_cot[...] = message(
        whole_rows * row_weight(at_rank[0]), halves * row_weight(at_rank[1] + at_rank[2])
    )

    pl.semaphore_wait(barrier, n_exp - 1 + 1 + n_y - 1)

    def scatter(src, dst, at):
        def one(i, carry):
            turn = n_exp - i
            half = lax.div(turn + 1, 2)
            odd = lax.rem(turn, 2)
            peer = lax.rem(me + odd * half + (1 - odd) * (n_exp - half), n_exp)
            pltpu.make_async_remote_copy(
                src_ref=src.at[peer],
                dst_ref=dst.at[me],
                send_sem=flat_send.at[at],
                recv_sem=flat_recv.at[at],
                device_id={"expert": peer},
                device_id_type=MESH,
            ).start()
            return carry

        lax.fori_loop(1, n_exp, one, 0)
        dst[me] = src[me]

    def wait_bytes(ref, sem):
        pltpu.make_async_copy(ref, ref, sem).wait()

    def wait_scatter(dst, at):
        wait_bytes(dst.at[pl.ds(0, n_exp - 1)], flat_recv.at[at])

    scatter(send_tok, got_tok, 0)
    scatter(send_cot, got_cot, 1)

    def matching(shape, row_dim):
        row = lax.broadcasted_iota(jnp.int32, shape, row_dim)
        col = lax.broadcasted_iota(jnp.int32, shape, 1 - row_dim)
        turn = jnp.bitwise_and(col, PAD - 1)
        first = jnp.right_shift(col, SHIFT) * cap
        ahead = jnp.where(first + turn == row, 1.0, 0.0)
        after = jnp.where(first + jnp.bitwise_and(turn, 1) + PAD == row, 1.0, 0.0)
        left = jnp.where(turn < 2, 1.0, 0.0)
        return [m.astype(BF16) for m in (ahead, after * left, after * (1.0 - left))]

    def flat(ref):
        return ref[...].astype(F32).reshape(lanes, width + piece).astype(BF16)

    def unfolded(picks, pieces):
        ends = [contract(picks[i], pieces[:, width:], 1, 0) for i in (1, 2)]
        return contract(picks[0], pieces[:, :width], 1, 0) + jnp.concatenate(ends, axis=1)

    pack = matching((rows, lanes), 0)
    wait_scatter(got_tok, 0)
    slot_in[...] = unfolded(pack, flat(got_tok)).astype(BF16)

    def put(kind, which, value):
        value = value.astype(BF16)
        for p, begin in enumerate(begins):
            for h in range(2):
                columns = value[:, h * cols + begin : h * cols + begin + widths[p]]
                products[2 * p + kind][h, :, which] = columns.reshape(n_y, block, widths[p])

    put(0, 0, contract(slot_in[...], wg[...], 1, 0))
    put(0, 1, contract(slot_in[...], wu[...], 1, 0))

    turns = near_order(n_y)

    def x_stage(at):
        for k in turns + [0]:
            b = y_at(k)
            pltpu.make_async_remote_copy(
                src_ref=products[at].at[other_x, b],
                dst_ref=landed[at].at[b],
                send_sem=x_send.at[at],
                recv_sem=x_recv.at[at, b],
                device_id={"dp": x_peer},
                device_id_type=MESH,
            ).start()

    def x_sum(at, b):
        wait_bytes(landed[at].at[b], x_recv.at[at, b])
        return (products[at][xx, b].astype(F32) + landed[at][b].astype(F32)).astype(BF16)

    def y_stage(at):
        for k in turns:
            b = y_at(k)
            passed[at][b] = x_sum(at, b)
            pltpu.make_async_remote_copy(
                src_ref=passed[at].at[b],
                dst_ref=terms[at].at[yy],
                send_sem=y_send.at[at],
                recv_sem=y_recv.at[at],
                device_id={"dp": b * 2 + xx},
                device_id_type=MESH,
            ).start()
        terms[at][yy] = x_sum(at, yy)

    def y_sum(at):
        wait_bytes(terms[at].at[pl.ds(0, n_y - 1)], y_recv.at[at])
        total = terms[at][0].astype(F32)
        for b in range(1, n_y):
            total = total + terms[at][b].astype(F32)
        return total

    def z_copy(p, m):
        return pltpu.make_async_remote_copy(
            src_ref=share[p].at[m],
            dst_ref=far[p].at[m],
            send_sem=z_send.at[3 * p + m],
            recv_sem=z_recv.at[3 * p + m],
            device_id={"expert": z_peer},
            device_id_type=MESH,
        )

    def forward(p):
        both = y_sum(2 * p)
        gate_pre, up_pre = both[0], both[1]
        sigma = 1.0 / (1.0 + jnp.exp(-gate_pre))
        share[p][0] = (gate_pre * sigma * up_pre).astype(BF16)
        z_copy(p, 0).start()
        return gate_pre, up_pre, sigma

    def backward(p, gate_pre, up_pre, sigma):
        upstream = y_sum(2 * p + 1)[0]
        share[p][1] = (upstream * up_pre * sigma * (1.0 + gate_pre * (1.0 - sigma))).astype(BF16)
        z_copy(p, 1).start()
        share[p][2] = (upstream * gate_pre * sigma).astype(BF16)
        z_copy(p, 2).start()

    x_stage(0)
    y_stage(0)
    wait_scatter(got_cot, 1)
    slot_back[...] = unfolded(pack, flat(got_cot)).astype(BF16)
    put(1, 0, contract(slot_back[...], wd[...], 1, 1))
    x_stage(1)
    x_stage(2)
    x_stage(3)
    y_stage(1)
    kept = forward(0)
    y_stage(2)
    backward(0, *kept)
    y_stage(3)
    kept = forward(1)

    row = (lax.broadcasted_iota(jnp.int32, (block, cols), 0) + yy * block).astype(F32)
    first = jnp.broadcast_to(limits[0, :1], (block, cols))
    last = jnp.broadcast_to(limits[1, :1], (block, cols))
    owned = jnp.where(row >= first, jnp.where(row < last, 1, 0), 0)

    def to_y(p, m):
        z_copy(p, m).wait_recv()
        mine = jnp.where(owned[:, : widths[p]] > 0, share[p][m].astype(F32), far[p][m].astype(F32))
        full[p][m, xx, yy] = mine.astype(BF16)
        for k in turns:
            b = y_at(k)
            pltpu.make_async_remote_copy(
                src_ref=full[p].at[m, xx, yy],
                dst_ref=full[p].at[m, xx, yy],
                send_sem=gy_send.at[3 * p + m],
                recv_sem=gy_recv.at[3 * p + m, yy],
                device_id={"dp": b * 2 + xx},
                device_id_type=MESH,
            ).start()
        to_x(p, m, yy)

    def to_x(p, m, b):
        pltpu.make_async_remote_copy(
            src_ref=full[p].at[m, xx, b],
            dst_ref=full[p].at[m, xx, b],
            send_sem=gx_send.at[3 * p + m],
            recv_sem=gx_recv.at[3 * p + m],
            device_id={"dp": x_peer},
            device_id_type=MESH,
        ).start()

    def pass_on(p, m):
        for k in reversed(turns):
            b = y_at(k)
            wait_bytes(full[p].at[m, xx, b], gy_recv.at[3 * p + m, b])
            to_x(p, m, b)

    def whole(p, m, h):
        return full[p][m, h].reshape(rows, widths[p])

    def span(p, h):
        return slice(h * cols + begins[p], h * cols + begins[p] + widths[p])

    pieces_of = [(p, h) for p in range(2) for h in range(2)]

    def product(m, mat, dim):
        for p in range(2):
            wait_bytes(full[p].at[m, other_x], gx_recv.at[3 * p + m])
        total = None
        for p, h in pieces_of:
            cut = mat[span(p, h), :] if dim == 0 else mat[:, span(p, h)]
            term = contract(whole(p, m, h), cut, 1, dim)
            total = term if total is None else total + term
        return total

    spread = matching((lanes, rows), 1)

    def give(value, src, dst, at):
        src[...] = message(*folded(spread, value.astype(BF16), 1))
        scatter(src, dst, at)

    to_y(0, 0)
    backward(1, *kept)
    to_y(0, 1)
    to_y(0, 2)
    pass_on(0, 0)
    pass_on(0, 1)
    to_y(1, 0)
    pass_on(0, 2)
    to_y(1, 1)
    to_y(1, 2)
    pass_on(1, 0)
    give(product(0, wd, 0), send_out, got_out, 2)
    pass_on(1, 1)
    pass_on(1, 2)
    dx = product(1, wg, 1)
    give(dx + product(2, wu, 1), send_dx, got_dx, 3)
    for p, h in pieces_of:
        ggrad[:, span(p, h)] = contract(slot_in[...], whole(p, 1, h), 0, 0).astype(BF16)
        ugrad[:, span(p, h)] = contract(slot_in[...], whole(p, 2, h), 0, 0).astype(BF16)
        dgrad[span(p, h), :] = contract(whole(p, 0, h), slot_back[...], 0, 0).astype(BF16)

    wait_scatter(got_out, 2)
    out_rows = flat(got_out)
    mixed[...] = (unfolded(w_high, out_rows) + unfolded(w_low, out_rows)).astype(BF16)
    wait_scatter(got_dx, 3)
    tgrad[...] = unfolded(own_sel, flat(got_dx)).astype(BF16)

    for at, src in enumerate((send_tok, send_cot, send_out, send_dx)):
        wait_bytes(src.at[pl.ds(0, n_exp - 1)], flat_send.at[at])
    for at in range(4):
        wait_bytes(products[at].at[0], x_send.at[at])
        wait_bytes(passed[at].at[pl.ds(0, n_y - 1)], y_send.at[at])
    for p in range(2):
        for m in range(3):
            z_copy(p, m).wait_send()
            wait_bytes(full[p].at[m, xx, pl.ds(0, n_y - 1)], gy_send.at[3 * p + m])
            wait_bytes(full[p].at[m, xx], gx_send.at[3 * p + m])


def hand_over(*refs):
    count = (len(refs) - 2) // 3
    src, dst, held = refs[:count], refs[count : 2 * count], refs[2 * count : 3 * count]
    taken, given = refs[3 * count :]
    first = [pltpu.make_async_copy(src[i], held[i], taken.at[i]) for i in range(count)]
    then = [pltpu.make_async_copy(held[i], dst[i], given.at[i]) for i in range(count)]
    for copy in first:
        copy.start()
    for i in range(count):
        first[i].wait()
        then[i].start()
    for copy in then:
        copy.wait()


def on_device(
    tokens, cotangent, expert_ids, gate_weights, slot_table, split_count, w_gate, w_up, w_down
):
    slot_count = slot_table.shape[0]
    expert_count = split_count.shape[0]
    token_count, top_k = expert_ids.shape
    width = tokens.shape[1]
    hidden_width = w_gate.shape[2]
    cap = max(2, (token_count * top_k + expert_count - 1) // expert_count)
    n_dp = lax.axis_size("dp")
    n_exp = slot_count
    n_y = n_dp // 2
    rows = n_exp * cap
    block = rows // n_y
    cols = hidden_width // 2
    lanes = n_exp * PAD

    vm = pl.BlockSpec(memory_space=pltpu.VMEM)
    message = pltpu.VMEM((n_exp, PAD, width + width // 2), BF16)

    widths = (cols - cols // 3, cols // 3)

    def halves(*lead):
        return [pltpu.VMEM((*lead, block, width), BF16) for width in widths]

    def kinds(*lead):
        pairs = zip(halves(*lead, 2), halves(*lead, 1), strict=True)
        return [buffer for pair in pairs for buffer in pair]

    dma = pltpu.SemaphoreType.DMA
    results = pl.pallas_call(
        functools.partial(layer_kernel, (n_dp, n_exp, cap, top_k)),
        out_shape=(
            jax.ShapeDtypeStruct((token_count, width), BF16),
            jax.ShapeDtypeStruct((token_count, width), BF16),
            jax.ShapeDtypeStruct((width, hidden_width), BF16),
            jax.ShapeDtypeStruct((width, hidden_width), BF16),
            jax.ShapeDtypeStruct((hidden_width, width), BF16),
        ),
        in_specs=[vm] * 9,
        out_specs=(vm,) * 5,
        scratch_shapes=[
            *([message] * 8),
            pltpu.VMEM((rows, width), BF16),
            pltpu.VMEM((rows, width), BF16),
            *([pltpu.VMEM((3, token_count, lanes), BF16)] * 3),
            pltpu.VMEM((128, 128), F32),
            pltpu.VMEM((2, 8, cols), F32),
            *kinds(2, n_y),
            *(kinds(n_y) * 3),
            *halves(3),
            *halves(3),
            *halves(3, 2, n_y),
            dma((4,)),
            dma((4,)),
            dma((4,)),
            dma((4, n_y)),
            dma((4,)),
            dma((4,)),
            dma((6,)),
            dma((6,)),
            dma((6,)),
            dma((6, n_y)),
            dma((6,)),
            dma((6,)),
        ],
        compiler_params=pltpu.CompilerParams(collective_id=0, has_side_effects=True),
        name="expert_layer",
    )(
        slot_table[None], split_count[None], expert_ids.T, gate_weights.T, tokens, cotangent,
        w_gate[0], w_up[0], w_down[0],
    )
    anywhere = pl.BlockSpec(memory_space=pl.ANY)
    mixed, tgrad, ggrad, ugrad, dgrad = pl.pallas_call(
        hand_over,
        out_shape=tuple(jax.ShapeDtypeStruct(r.shape, r.dtype) for r in results),
        in_specs=[anywhere] * 5,
        out_specs=(anywhere,) * 5,
        scratch_shapes=[*(pltpu.VMEM(r.shape, r.dtype) for r in results), dma((5,)), dma((5,))],
        name="hand_over",
    )(*results)
    return mixed, tgrad, ggrad[None], ugrad[None], dgrad[None]


def solution(mesh):
    return jax.shard_map(
        on_device,
        mesh=mesh,
        in_specs=(
            P("expert", "dp"),
            P("expert", "dp"),
            P("expert", None),
            P("expert", None),
            P(),
            P(),
            P("expert", "dp", None),
            P("expert", "dp", None),
            P("expert", None, "dp"),
        ),
        out_specs=(
            P("expert", "dp"),
            P("expert", "dp"),
            P("expert", "dp", None),
            P("expert", "dp", None),
            P("expert", None, "dp"),
        ),
        check_vma=False,
    )
```

```python
import functools

import jax
import jax.numpy as jnp
from jax import lax
from jax.experimental import pallas as pl
from jax.experimental.pallas import tpu as pltpu
from jax.sharding import PartitionSpec as P

MESH = pl.DeviceIdType.MESH
BF16 = jnp.bfloat16
F32 = jnp.float32
PAD = 4
SHIFT = 2


def contract(a, b, da, db):
    return lax.dot_general(a, b, (((da,), (db,)), ((), ())), preferred_element_type=F32)


def near_order(count):
    return sorted(range(1, count), key=lambda k: (-min(k, count - k), k))


def layer_kernel(
    dims,
    table, splits, ids, gates, tok, cot, wg, wu, wd,
    mixed, tgrad, ggrad, ugrad, dgrad,
    send_tok, send_cot, send_out, send_dx, got_tok, got_cot, got_out, got_dx,
    slot_in, slot_back, w_high, w_low, own_sel, turned, limits,
    *rest,
):
    products, landed, passed, terms = (rest[4 * i : 4 * i + 4] for i in range(4))
    share, far, full = (rest[16 + 2 * i : 18 + 2 * i] for i in range(3))
    (
        flat_send, flat_recv, x_send, x_recv, y_send, y_recv, z_send, z_recv,
        gy_send, gy_recv, gx_send, gx_recv,
    ) = rest[22:]
    n_dp, n_exp, cap, top = dims
    assert cap == PAD + 2
    n_y = n_dp // 2
    tokens, width = tok.shape
    rows = n_exp * cap
    lanes = n_exp * PAD
    block = share[0].shape[1]
    widths = [ref.shape[2] for ref in share]
    cols = sum(widths)
    begins = [0, widths[0]]
    me = lax.axis_index("expert")
    place = lax.axis_index("dp")
    yy = lax.div(place, 2)
    xx = lax.rem(place, 2)
    other_x = 1 - xx
    x_peer = yy * 2 + other_x
    z_peer = lax.rem(me + n_exp // 2, n_exp)

    def y_at(k):
        return lax.rem(yy + k, n_y)

    barrier = pltpu.get_barrier_semaphore()

    def greet(k, carry):
        pl.semaphore_signal(
            barrier, inc=1, device_id={"expert": lax.rem(me + k, n_exp)}, device_id_type=MESH
        )
        return carry

    lax.fori_loop(1, n_exp, greet, 0)
    pl.semaphore_signal(barrier, inc=1, device_id={"dp": x_peer}, device_id_type=MESH)
    for k in range(1, n_y):
        pl.semaphore_signal(barrier, inc=1, device_id={"dp": y_at(k) * 2 + xx}, device_id_type=MESH)

    def lane_of_slot(shift):
        slot = lax.broadcasted_iota(jnp.int32, (n_exp, lanes), 0) + shift
        slot = jnp.where(slot >= n_exp, slot - n_exp, slot)
        lane = jnp.right_shift(lax.broadcasted_iota(jnp.int32, (n_exp, lanes), 1), SHIFT)
        return jnp.where(slot == lane, 1.0, 0.0).astype(BF16)

    def small(ref):
        return jnp.broadcast_to(ref[...].astype(F32), (8, ref.shape[1])).astype(BF16)

    slot_expert = contract(small(table), lane_of_slot(0), 1, 0)
    other_expert = contract(small(table), lane_of_slot(n_exp // 2), 1, 0)
    experts = splits.shape[1]
    expert = lax.broadcasted_iota(jnp.int32, (experts, lanes), 0).astype(F32)
    named = jnp.where(expert == jnp.broadcast_to(slot_expert[:1], (experts, lanes)), 1.0, 0.0)
    split_at = contract(small(splits), named.astype(BF16), 1, 0)
    lane = lax.broadcasted_iota(jnp.int32, (8, lanes), 1)
    alone = slot_expert != other_expert
    start = jnp.where(alone, 0.0, jnp.where(lane < lanes // 2, 0.0, split_at))
    end = jnp.where(alone, float(n_exp), jnp.where(lane < lanes // 2, split_at, float(n_exp)))
    mine = me.astype(F32)
    lane_chosen = jnp.where(start <= mine, jnp.where(mine < end, 1.0, 0.0), 0.0)
    for i, limit in enumerate((start, end)):
        at_me = jnp.sum(jnp.where(lane == me * PAD, limit, 0.0), axis=1, keepdims=True)
        limits[i] = jnp.broadcast_to(at_me * cap, (8, cols))

    turned[...] = jnp.zeros(turned.shape, F32)
    turned[0:top, 0:tokens] = ids[...].astype(F32)
    turned[top : 2 * top, 0:tokens] = gates[...]
    columns = jnp.transpose(turned[...])[:tokens]
    shape = (tokens, lanes)
    held = jnp.zeros(shape, F32)
    weight = jnp.zeros(shape, F32)
    wanted = jnp.broadcast_to(slot_expert[:1], shape)
    for k in range(top):
        hit = jnp.broadcast_to(columns[:, k : k + 1], shape) == wanted
        held = jnp.where(hit, 1.0, held)
        weight = jnp.where(hit, jnp.broadcast_to(columns[:, top + k : top + k + 1], shape), weight)
    t_row = lax.broadcasted_iota(jnp.int32, (tokens, tokens), 0)
    t_col = lax.broadcasted_iota(jnp.int32, (tokens, tokens), 1)
    earlier = jnp.where(t_col < t_row, 1.0, 0.0).astype(BF16)
    position = contract(earlier, held.astype(BF16), 1, 0)
    turn = jnp.bitwise_and(lax.broadcasted_iota(jnp.int32, shape, 1), PAD - 1)
    ranks = (turn, jnp.bitwise_and(turn, 1) + PAD)
    at_rank = [jnp.where(position == rank.astype(F32), held, 0.0) for rank in ranks]
    left = jnp.where(turn < 2, 1.0, 0.0)
    at_rank = [at_rank[0], at_rank[1] * left, at_rank[1] * (1.0 - left)]
    chosen = jnp.broadcast_to(lane_chosen[:1], shape)
    for i, at in enumerate(at_rank):
        own_weight = at * chosen * weight
        high = own_weight.astype(BF16)
        w_high[i] = high
        w_low[i] = (own_weight - high.astype(F32)).astype(BF16)
        own_sel[i] = (at * chosen).astype(BF16)
    piece = width // 2

    def folded(picks, value, da):
        whole_rows = contract(picks[0], value, da, 0)
        halves = contract(picks[1], value[:, :piece], da, 0) + contract(picks[2], value[:, piece:], da, 0)
        return whole_rows, halves

    def message(whole_rows, halves):
        both = jnp.concatenate([whole_rows, halves], axis=1)
        return both.reshape(n_exp, PAD, width + piece).astype(BF16)

    picks = [at.astype(BF16) for at in at_rank]
    send_tok[...] = message(*folded(picks, tok[...], 0))

    def row_weight(at):
        row = jnp.sum(at * weight, axis=0, keepdims=True)
        return jnp.transpose(jnp.broadcast_to(row, (128, lanes)))[:, :1]

    whole_rows, halves = folded(picks, cot[...], 0)
    send_cot[...] = message(
        whole_rows * row_weight(at_rank[0]), halves * row_weight(at_rank[1] + at_rank[2])
    )

    pl.semaphore_wait(barrier, n_exp - 1 + 1 + n_y - 1)

    def scatter(src, dst, at):
        def one(i, carry):
            turn = n_exp - i
            half = lax.div(turn + 1, 2)
            odd = lax.rem(turn, 2)
            peer = lax.rem(me + odd * half + (1 - odd) * (n_exp - half), n_exp)
            pltpu.make_async_remote_copy(
                src_ref=src.at[peer],
                dst_ref=dst.at[me],
                send_sem=flat_send.at[at],
                recv_sem=flat_recv.at[at],
                device_id={"expert": peer},
                device_id_type=MESH,
            ).start()
            return carry

        lax.fori_loop(1, n_exp, one, 0)
        dst[me] = src[me]

    def wait_bytes(ref, sem):
        pltpu.make_async_copy(ref, ref, sem).wait()

    def wait_scatter(dst, at):
        wait_bytes(dst.at[pl.ds(0, n_exp - 1)], flat_recv.at[at])

    scatter(send_tok, got_tok, 0)
    scatter(send_cot, got_cot, 1)

    def matching(shape, row_dim):
        row = lax.broadcasted_iota(jnp.int32, shape, row_dim)
        col = lax.broadcasted_iota(jnp.int32, shape, 1 - row_dim)
        turn = jnp.bitwise_and(col, PAD - 1)
        first = jnp.right_shift(col, SHIFT) * cap
        ahead = jnp.where(first + turn == row, 1.0, 0.0)
        after = jnp.where(first + jnp.bitwise_and(turn, 1) + PAD == row, 1.0, 0.0)
        left = jnp.where(turn < 2, 1.0, 0.0)
        return [m.astype(BF16) for m in (ahead, after * left, after * (1.0 - left))]

    def flat(ref):
        return ref[...].astype(F32).reshape(lanes, width + piece).astype(BF16)

    def unfolded(picks, pieces):
        ends = [contract(picks[i], pieces[:, width:], 1, 0) for i in (1, 2)]
        return contract(picks[0], pieces[:, :width], 1, 0) + jnp.concatenate(ends, axis=1)

    pack = matching((rows, lanes), 0)
    wait_scatter(got_tok, 0)
    slot_in[...] = unfolded(pack, flat(got_tok)).astype(BF16)

    def put(kind, which, value):
        value = value.astype(BF16)
        for p, begin in enumerate(begins):
            for h in range(2):
                columns = value[:, h * cols + begin : h * cols + begin + widths[p]]
                products[2 * p + kind][h, :, which] = columns.reshape(n_y, block, widths[p])

    put(0, 0, contract(slot_in[...], wg[...], 1, 0))
    put(0, 1, contract(slot_in[...], wu[...], 1, 0))

    turns = near_order(n_y)

    def x_stage(at):
        for k in turns + [0]:
            b = y_at(k)
            pltpu.make_async_remote_copy(
                src_ref=products[at].at[other_x, b],
                dst_ref=landed[at].at[b],
                send_sem=x_send.at[at],
                recv_sem=x_recv.at[at, b],
                device_id={"dp": x_peer},
                device_id_type=MESH,
            ).start()

    def x_sum(at, b):
        wait_bytes(landed[at].at[b], x_recv.at[at, b])
        return (products[at][xx, b].astype(F32) + landed[at][b].astype(F32)).astype(BF16)

    def y_stage(at):
        for k in turns:
            b = y_at(k)
            passed[at][b] = x_sum(at, b)
            pltpu.make_async_remote_copy(
                src_ref=passed[at].at[b],
                dst_ref=terms[at].at[yy],
                send_sem=y_send.at[at],
                recv_sem=y_recv.at[at],
                device_id={"dp": b * 2 + xx},
                device_id_type=MESH,
            ).start()
        terms[at][yy] = x_sum(at, yy)

    def y_sum(at):
        wait_bytes(terms[at].at[pl.ds(0, n_y - 1)], y_recv.at[at])
        total = terms[at][0].astype(F32)
        for b in range(1, n_y):
            total = total + terms[at][b].astype(F32)
        return total

    def z_copy(p, m):
        return pltpu.make_async_remote_copy(
            src_ref=share[p].at[m],
            dst_ref=far[p].at[m],
            send_sem=z_send.at[3 * p + m],
            recv_sem=z_recv.at[3 * p + m],
            device_id={"expert": z_peer},
            device_id_type=MESH,
        )

    def forward(p):
        both = y_sum(2 * p)
        gate_pre, up_pre = both[0], both[1]
        sigma = 1.0 / (1.0 + jnp.exp(-gate_pre))
        share[p][0] = (gate_pre * sigma * up_pre).astype(BF16)
        z_copy(p, 0).start()
        return gate_pre, up_pre, sigma

    def backward(p, gate_pre, up_pre, sigma):
        upstream = y_sum(2 * p + 1)[0]
        share[p][1] = (upstream * up_pre * sigma * (1.0 + gate_pre * (1.0 - sigma))).astype(BF16)
        z_copy(p, 1).start()
        share[p][2] = (upstream * gate_pre * sigma).astype(BF16)
        z_copy(p, 2).start()

    x_stage(0)
    x_stage(2)
    y_stage(0)
    wait_scatter(got_cot, 1)
    slot_back[...] = unfolded(pack, flat(got_cot)).astype(BF16)
    put(1, 0, contract(slot_back[...], wd[...], 1, 1))
    x_stage(1)
    x_stage(3)
    y_stage(2)
    kept = [forward(0)]
    y_stage(1)
    kept.append(forward(1))
    y_stage(3)
    backward(0, *kept[0])

    row = (lax.broadcasted_iota(jnp.int32, (block, cols), 0) + yy * block).astype(F32)
    first = jnp.broadcast_to(limits[0, :1], (block, cols))
    last = jnp.broadcast_to(limits[1, :1], (block, cols))
    owned = jnp.where(row >= first, jnp.where(row < last, 1, 0), 0)

    def to_y(p, m):
        z_copy(p, m).wait_recv()
        mine = jnp.where(owned[:, : widths[p]] > 0, share[p][m].astype(F32), far[p][m].astype(F32))
        full[p][m, xx, yy] = mine.astype(BF16)
        for k in turns:
            b = y_at(k)
            pltpu.make_async_remote_copy(
                src_ref=full[p].at[m, xx, yy],
                dst_ref=full[p].at[m, xx, yy],
                send_sem=gy_send.at[3 * p + m],
                recv_sem=gy_recv.at[3 * p + m, yy],
                device_id={"dp": b * 2 + xx},
                device_id_type=MESH,
            ).start()
        to_x(p, m, yy)

    def to_x(p, m, b):
        pltpu.make_async_remote_copy(
            src_ref=full[p].at[m, xx, b],
            dst_ref=full[p].at[m, xx, b],
            send_sem=gx_send.at[3 * p + m],
            recv_sem=gx_recv.at[3 * p + m],
            device_id={"dp": x_peer},
            device_id_type=MESH,
        ).start()

    def pass_on(p, m):
        for k in reversed(turns):
            b = y_at(k)
            wait_bytes(full[p].at[m, xx, b], gy_recv.at[3 * p + m, b])
            to_x(p, m, b)

    def whole(p, m, h):
        return full[p][m, h].reshape(rows, widths[p])

    def span(p, h):
        return slice(h * cols + begins[p], h * cols + begins[p] + widths[p])

    pieces_of = [(p, h) for p in range(2) for h in range(2)]

    def product(m, mat, dim):
        for p in range(2):
            wait_bytes(full[p].at[m, other_x], gx_recv.at[3 * p + m])
        total = None
        for p, h in pieces_of:
            cut = mat[span(p, h), :] if dim == 0 else mat[:, span(p, h)]
            term = contract(whole(p, m, h), cut, 1, dim)
            total = term if total is None else total + term
        return total

    spread = matching((lanes, rows), 1)

    def give(value, src, dst, at):
        src[...] = message(*folded(spread, value.astype(BF16), 1))
        scatter(src, dst, at)

    to_y(0, 0)
    backward(1, *kept[1])
    to_y(1, 0)
    pass_on(0, 0)
    to_y(0, 1)
    to_y(0, 2)
    pass_on(1, 0)
    pass_on(0, 1)
    to_y(1, 1)
    give(product(0, wd, 0), send_out, got_out, 2)
    pass_on(0, 2)
    to_y(1, 2)
    pass_on(1, 1)
    pass_on(1, 2)
    dx = product(1, wg, 1)
    give(dx + product(2, wu, 1), send_dx, got_dx, 3)
    for p, h in pieces_of:
        ggrad[:, span(p, h)] = contract(slot_in[...], whole(p, 1, h), 0, 0).astype(BF16)
        ugrad[:, span(p, h)] = contract(slot_in[...], whole(p, 2, h), 0, 0).astype(BF16)
        dgrad[span(p, h), :] = contract(whole(p, 0, h), slot_back[...], 0, 0).astype(BF16)

    wait_scatter(got_out, 2)
    out_rows = flat(got_out)
    mixed[...] = (unfolded(w_high, out_rows) + unfolded(w_low, out_rows)).astype(BF16)
    wait_scatter(got_dx, 3)
    tgrad[...] = unfolded(own_sel, flat(got_dx)).astype(BF16)

    for at, src in enumerate((send_tok, send_cot, send_out, send_dx)):
        wait_bytes(src.at[pl.ds(0, n_exp - 1)], flat_send.at[at])
    for at in range(4):
        wait_bytes(products[at].at[0], x_send.at[at])
        wait_bytes(passed[at].at[pl.ds(0, n_y - 1)], y_send.at[at])
    for p in range(2):
        for m in range(3):
            z_copy(p, m).wait_send()
            wait_bytes(full[p].at[m, xx, pl.ds(0, n_y - 1)], gy_send.at[3 * p + m])
            wait_bytes(full[p].at[m, xx], gx_send.at[3 * p + m])


def hand_over(*refs):
    count = (len(refs) - 2) // 3
    src, dst, held = refs[:count], refs[count : 2 * count], refs[2 * count : 3 * count]
    taken, given = refs[3 * count :]
    first = [pltpu.make_async_copy(src[i], held[i], taken.at[i]) for i in range(count)]
    then = [pltpu.make_async_copy(held[i], dst[i], given.at[i]) for i in range(count)]
    for copy in first:
        copy.start()
    for i in range(count):
        first[i].wait()
        then[i].start()
    for copy in then:
        copy.wait()


def on_device(
    tokens, cotangent, expert_ids, gate_weights, slot_table, split_count, w_gate, w_up, w_down
):
    slot_count = slot_table.shape[0]
    expert_count = split_count.shape[0]
    token_count, top_k = expert_ids.shape
    width = tokens.shape[1]
    hidden_width = w_gate.shape[2]
    cap = max(2, (token_count * top_k + expert_count - 1) // expert_count)
    n_dp = lax.axis_size("dp")
    n_exp = slot_count
    n_y = n_dp // 2
    rows = n_exp * cap
    block = rows // n_y
    cols = hidden_width // 2
    lanes = n_exp * PAD

    vm = pl.BlockSpec(memory_space=pltpu.VMEM)
    message = pltpu.VMEM((n_exp, PAD, width + width // 2), BF16)

    widths = (cols - cols // 3, cols // 3)

    def halves(*lead):
        return [pltpu.VMEM((*lead, block, width), BF16) for width in widths]

    def kinds(*lead):
        pairs = zip(halves(*lead, 2), halves(*lead, 1), strict=True)
        return [buffer for pair in pairs for buffer in pair]

    dma = pltpu.SemaphoreType.DMA
    results = pl.pallas_call(
        functools.partial(layer_kernel, (n_dp, n_exp, cap, top_k)),
        out_shape=(
            jax.ShapeDtypeStruct((token_count, width), BF16),
            jax.ShapeDtypeStruct((token_count, width), BF16),
            jax.ShapeDtypeStruct((width, hidden_width), BF16),
            jax.ShapeDtypeStruct((width, hidden_width), BF16),
            jax.ShapeDtypeStruct((hidden_width, width), BF16),
        ),
        in_specs=[vm] * 9,
        out_specs=(vm,) * 5,
        scratch_shapes=[
            *([message] * 8),
            pltpu.VMEM((rows, width), BF16),
            pltpu.VMEM((rows, width), BF16),
            *([pltpu.VMEM((3, token_count, lanes), BF16)] * 3),
            pltpu.VMEM((128, 128), F32),
            pltpu.VMEM((2, 8, cols), F32),
            *kinds(2, n_y),
            *(kinds(n_y) * 3),
            *halves(3),
            *halves(3),
            *halves(3, 2, n_y),
            dma((4,)),
            dma((4,)),
            dma((4,)),
            dma((4, n_y)),
            dma((4,)),
            dma((4,)),
            dma((6,)),
            dma((6,)),
            dma((6,)),
            dma((6, n_y)),
            dma((6,)),
            dma((6,)),
        ],
        compiler_params=pltpu.CompilerParams(collective_id=0, has_side_effects=True),
        name="expert_layer",
    )(
        slot_table[None], split_count[None], expert_ids.T, gate_weights.T, tokens, cotangent,
        w_gate[0], w_up[0], w_down[0],
    )
    anywhere = pl.BlockSpec(memory_space=pl.ANY)
    mixed, tgrad, ggrad, ugrad, dgrad = pl.pallas_call(
        hand_over,
        out_shape=tuple(jax.ShapeDtypeStruct(r.shape, r.dtype) for r in results),
        in_specs=[anywhere] * 5,
        out_specs=(anywhere,) * 5,
        scratch_shapes=[*(pltpu.VMEM(r.shape, r.dtype) for r in results), dma((5,)), dma((5,))],
        name="hand_over",
    )(*results)
    return mixed, tgrad, ggrad[None], ugrad[None], dgrad[None]


def solution(mesh):
    return jax.shard_map(
        on_device,
        mesh=mesh,
        in_specs=(
            P("expert", "dp"),
            P("expert", "dp"),
            P("expert", None),
            P("expert", None),
            P(),
            P(),
            P("expert", "dp", None),
            P("expert", "dp", None),
            P("expert", None, "dp"),
        ),
        out_specs=(
            P("expert", "dp"),
            P("expert", "dp"),
            P("expert", "dp", None),
            P("expert", "dp", None),
            P("expert", None, "dp"),
        ),
        check_vma=False,
    )
```
